32 devices in a mesh: dp: 8 (over z, y), fsdp: 4 (over x, core).
Axes of the slice: x: 2, y: 2, z: 4, core: 2. Of those that a mesh axis runs over, the one named last changes fastest.
Arguments:
- tokens: bfloat16 [65536, 384], P(('dp', 'fsdp')), may hold values from -6 to 6
- cotangent: bfloat16 [65536, 384], P(('dp', 'fsdp')), may hold values from -6 to 6
- image_lengths: int32 [32, 112], P(('dp', 'fsdp')), may hold values from 0 to 66, as said below
- segment_ids: int32 [65536], P(('dp', 'fsdp')), may hold values from 0 to 112, as said below
- w_qkv: bfloat16 [442368], P(('dp', 'fsdp')), may hold values from -0.3125 to 0.3125
- w_out: bfloat16 [147456], P(('dp', 'fsdp')), may hold values from -1.75 to 1.75
- w_up: bfloat16 [589824], P(('dp', 'fsdp')), may hold values from -0.3125 to 0.3125
- w_down: bfloat16 [589824], P(('dp', 'fsdp')), may hold values from -0.15625 to 0.15625
- small_params: bfloat16 [4608], P(('dp', 'fsdp'))
Outputs:
- output: bfloat16 [65536, 384], P(('dp', 'fsdp'))
- input_grad: bfloat16 [65536, 384], P(('dp', 'fsdp'))
- grad_qkv: float32 [442368], P(('dp', 'fsdp'))
- grad_out: float32 [147456], P(('dp', 'fsdp'))
- grad_up: float32 [589824], P(('dp', 'fsdp'))
- grad_down: float32 [589824], P(('dp', 'fsdp'))
- grad_small: float32 [4608], P(('dp', 'fsdp'))
The draws below stay inside these ranges and needn't reach their ends.
Inputs may be any that keep to these rules, and one draw needn't show every extreme that they name: `image_lengths`: row p lists pack p's images in order, then zeros. The first image of every pack has 66 tokens, and every other image but a pack's last has 18 tokens or more. A pack's lengths sum to at least 1843 and below 2048, except in one pack, which holds 112 images and sums to 2048. `segment_ids`: token t of pack p carries the number of pack p's images that end at or before t; padding after the last image carries 112.
All inputs are finite; a program needn't handle non-finite values.
Results may differ from the reference program's by a relative error of at most 0.011.
Values may be sent and summed in bfloat16 or wider, within the bound.
A program may use at most 128 MiB of HBM per device.

```python
import jax
import jax.numpy as jnp
from jax import lax

HEADS = 6
HEAD_DIM = 64
FF = 1536
D = 384
TOK_DEV = 2048
MIN_IMG = 18
MAX_IMG = 66
SLOTS = 112
PACKS = 32
TOKENS = 65536


def pack_layout(key):
    base = jax.random.fold_in(key, 17)
    key_len, key_fill, key_full = jax.random.split(base, 3)
    slot_ids = jnp.arange(SLOTS, dtype=jnp.int32)
    pack_ids = jnp.arange(PACKS, dtype=jnp.int32)
    chosen = jax.random.randint(key_full, (), 0, PACKS, dtype=jnp.int32)
    drawn = jax.random.randint(key_len, (PACKS, SLOTS), MIN_IMG, MAX_IMG + 1, dtype=jnp.int32)
    drawn = jnp.where(pack_ids[:, None] == chosen, MIN_IMG, drawn)
    drawn = jnp.where(slot_ids[None, :] == 0, MAX_IMG, drawn)
    target = jax.random.randint(key_fill, (PACKS,), 9 * TOK_DEV // 10, TOK_DEV, dtype=jnp.int32)
    target = jnp.where(pack_ids == chosen, TOK_DEV, target)
    ending = jnp.cumsum(drawn, axis=1)
    kept = ending <= target[:, None]
    lengths = jnp.where(kept, drawn, 0)
    remain = target - jnp.sum(lengths, axis=1)
    kept_count = jnp.sum(kept.astype(jnp.int32), axis=1)
    lengths = lengths + jnp.where(slot_ids[None, :] == kept_count[:, None], remain[:, None], 0)
    return lengths.astype(jnp.int32)


def draw_image_lengths(key, part):
    return pack_layout(key)


def draw_segment_ids(key, part):
    lengths = pack_layout(key)
    ending = jnp.cumsum(lengths, axis=1)
    positions = jnp.arange(TOK_DEV, dtype=jnp.int32)
    segments = jnp.sum((ending[:, None, :] <= positions[None, :, None]).astype(jnp.int32), axis=2)
    return segments.reshape(PACKS * TOK_DEV).astype(jnp.int32)


def draw_small_params(key, part):
    key_gain, key_bias = jax.random.split(jax.random.fold_in(key, 3))
    gains = jnp.exp(jax.random.uniform(key_gain, (2 * D,), jnp.float32, -0.4, 0.4))
    biases = 0.5 * jax.random.normal(key_bias, (6 * D + FF,), jnp.float32)
    return jnp.concatenate([gains, biases]).astype(jnp.bfloat16)


def steps_of(key, dims, cuts, low, largest):
    factor_of = 1.0
    for dim, shards_of in cuts:
        draws = jax.random.uniform(jax.random.fold_in(jax.random.fold_in(key, 6), dim), (shards_of,), jnp.float32, low / len(cuts), largest / len(cuts))
        factor_of = factor_of * jnp.repeat(jnp.exp(draws), dims[dim] // shards_of).reshape((-1,) + (1,) * (len(dims) - 1 - dim))
    return factor_of


def bell_draw(key, shape, scale, bound, shards=(), kind=jnp.bfloat16):
    values = scale * jax.random.normal(key, shape, jnp.float32)
    if shards:
        values = values * steps_of(key, shape, shards, -0.22, 0.18)
    return jnp.clip(values, -bound, bound).astype(kind)


def setup_inputs(seed: int = 0) -> dict:
    keys = jax.random.split(jax.random.key(seed), 10)
    return {
        "tokens": bell_draw(keys[0], (TOKENS, D), 1.0, 6.0, ((0, 32),)),
        "cotangent": bell_draw(keys[1], (TOKENS, D), 1.0, 6.0, ((0, 32),)),
        "image_lengths": draw_image_lengths(jax.random.fold_in(keys[9], 71), 0),
        "segment_ids": draw_segment_ids(jax.random.fold_in(keys[9], 71), 0),
        "w_qkv": bell_draw(keys[4], (3 * D * D,), D ** -0.5, 0.3125, ((0, 32),)),
        "w_out": bell_draw(keys[5], (D * D,), (D // 32) ** -0.5, 1.75, ((0, 32),)),
        "w_up": bell_draw(keys[6], (D * FF,), D ** -0.5, 0.3125, ((0, 32),)),
        "w_down": bell_draw(keys[7], (FF * D,), FF ** -0.5, 0.15625, ((0, 32),)),
        "small_params": draw_small_params(jax.random.fold_in(keys[9], 71), 0),
    }


norm_eps = 1e-06
masked_score = -1e+30

@jax.custom_vjp
def low(v):
    return lax.optimization_barrier(v.astype(jnp.bfloat16)).astype(jnp.float32)

@jax.custom_vjp
def low_back(v):
    return v

def low_keep(v):
    return (low(v), None)

def low_pass(kept, grad):
    return (grad,)

def back_keep(v):
    return (v, None)

def back_low(kept, grad):
    return (low(grad),)
low.defvjp(low_keep, low_pass)
low_back.defvjp(back_keep, back_low)

def matmul(left_side, right_side):
    return jnp.dot(left_side, right_side, precision=lax.Precision.HIGHEST, preferred_element_type=jnp.float32)

def layer_norm(inputs, gain, shift):
    center = lax.optimization_barrier(jnp.mean(inputs, axis=-1, keepdims=True))
    offset = inputs - center
    spread = lax.optimization_barrier(jnp.mean(offset * offset, axis=-1, keepdims=True))
    return offset * lax.rsqrt(spread + norm_eps) * gain + shift

def split_small(small_all):
    model_width = HEADS * HEAD_DIM
    pieces = tuple((small_all[member * model_width:(member + 1) * model_width] for member in range(8)))
    return pieces + (small_all[8 * model_width:],)

def layer(hidden_in, segments, filled, qkv_mat, out_mat, up_mat, down_mat, small_all):
    gain_one, gain_two, bias_one, bias_two, bias_query, bias_value, bias_out, bias_down, bias_up = split_small(small_all)
    model_width = HEADS * HEAD_DIM
    rows_count = hidden_in.shape[0]
    normed = low(layer_norm(hidden_in, gain_one, bias_one))
    projected = low_back(matmul(normed, qkv_mat))
    queries = low(projected[:, :model_width] + bias_query).reshape(rows_count, HEADS, HEAD_DIM)
    keys_all = low(projected[:, model_width:2 * model_width]).reshape(rows_count, HEADS, HEAD_DIM)
    values_all = low(projected[:, 2 * model_width:] + bias_value).reshape(rows_count, HEADS, HEAD_DIM)
    scores = low_back(jnp.einsum('qhd,khd->hqk', queries, keys_all, precision=lax.Precision.HIGHEST) * HEAD_DIM ** (-0.5))
    allowed = segments[:, None] == segments[None, :]
    scores = jnp.where(allowed[None], scores, masked_score)
    peak = lax.optimization_barrier(jnp.max(scores, axis=-1, keepdims=True))
    exponent = jnp.exp(scores - peak)
    probs = low(exponent / lax.optimization_barrier(jnp.sum(exponent, axis=-1, keepdims=True)))
    attended = low_back(jnp.einsum('hqk,khd->qhd', probs, values_all, precision=lax.Precision.HIGHEST)).reshape(rows_count, model_width)
    mixed = hidden_in + low_back(matmul(low(attended), out_mat)) + bias_out
    normed_two = low(layer_norm(mixed, gain_two, bias_two))
    upward = low_back(matmul(normed_two, up_mat)) + bias_up
    activated = low(jax.nn.gelu(upward, approximate=False))
    result = mixed + low_back(matmul(activated, down_mat)) + bias_down
    return result * filled[:, None]

def reference(tokens, cotangent, image_lengths, segment_ids, w_qkv, w_out, w_up, w_down, small_params):
    model_width = HEADS * HEAD_DIM
    weights = (w_qkv.astype(jnp.float32).reshape(model_width, 3 * model_width), w_out.astype(jnp.float32).reshape(model_width, model_width), w_up.astype(jnp.float32).reshape(model_width, FF), w_down.astype(jnp.float32).reshape(FF, model_width), small_params.astype(jnp.float32))
    packed = tokens.astype(jnp.float32).reshape(PACKS, TOK_DEV, model_width)
    upstream = cotangent.astype(jnp.float32).reshape(PACKS, TOK_DEV, model_width)
    segments = segment_ids.reshape(PACKS, TOK_DEV)
    positions = jnp.arange(TOK_DEV, dtype=jnp.int32)

    def one_pack(totals, inputs_pack):
        hidden_in, grad_in, lengths, seg_row = inputs_pack
        filled = (positions < jnp.sum(lengths)).astype(jnp.float32)

        def forward(hidden, qkv_mat, out_mat, up_mat, down_mat, small_all):
            return layer(hidden, seg_row, filled, qkv_mat, out_mat, up_mat, down_mat, small_all)
        result, pullback = jax.vjp(forward, hidden_in, weights[0], weights[1], weights[2], weights[3], weights[4])
        gradients = pullback(grad_in)
        updated = tuple((summed + gradient for summed, gradient in zip(totals, gradients[1:])))
        return (updated, (result.astype(jnp.bfloat16), gradients[0].astype(jnp.bfloat16)))
    initial = tuple((jnp.zeros_like(weight) for weight in weights))
    totals, (outputs, input_grads) = lax.scan(one_pack, initial, (packed, upstream, image_lengths, segments))
    return (outputs.reshape(TOKENS, model_width), input_grads.reshape(TOKENS, model_width), totals[0].reshape(-1), totals[1].reshape(-1), totals[2].reshape(-1), totals[3].reshape(-1), totals[4])
```

```python
import functools

import jax
import jax.numpy as jnp
from jax import lax
from jax.experimental import pallas as pl
from jax.experimental.pallas import tpu as pltpu
from jax.sharding import PartitionSpec as P

HEADS = 6
HEAD_DIM = 64
FF = 1536
D = HEADS * HEAD_DIM
PAIRS = D // 128
MAX_IMG = 66
NORM_EPS = 1e-06
MASKED = -1e30
F32 = jnp.float32
BF16 = jnp.bfloat16

GAIN1, GAIN2, BIAS1, BIAS2, BQ, BV, BOUT, BDOWN, BUP = range(9)
SMALL_ROWS = 16

TQ = 128
MARGIN = 16 * ((MAX_IMG - 1 + 15) // 16)
WIN = TQ + 2 * MARGIN


def nn(a, b):
    return jnp.dot(a, b, preferred_element_type=F32)


def nt(a, b):
    return lax.dot_general(a, b, (((1,), (1,)), ((), ())), preferred_element_type=F32)


def tn(a, b):
    return lax.dot_general(a, b, (((0,), (0,)), ((), ())), preferred_element_type=F32)


def normalize(x):
    center = jnp.mean(x, axis=-1, keepdims=True)
    off = x - center
    r = lax.rsqrt(jnp.mean(off * off, axis=-1, keepdims=True) + NORM_EPS)
    return off * r, r


def norm_back(grad, gain, xhat, r):
    gx = grad * gain
    return r * (gx - jnp.mean(gx, axis=-1, keepdims=True) - xhat * jnp.mean(gx * xhat, axis=-1, keepdims=True))


def colsum(x):
    return jnp.sum(x, axis=0, keepdims=True)


def gelu_parts(u):
    e = jnp.exp(u * u * -0.5)
    t = 1.0 / (1.0 + jnp.abs(u) * (0.3275911 * 0.7071067811865476))
    poly = t * (0.127414796 + t * (-0.142248368 + t * (0.7107068705 + t * (-0.7265760135 + t * 0.5307027145))))
    tail = poly * e
    cdf = jnp.where(u >= 0.0, 1.0 - tail, tail)
    return cdf, e * 0.3989422804014327


def half_masks(rows):
    lane = lax.broadcasted_iota(jnp.int32, (rows, 128), 1)
    low = (lane < HEAD_DIM).astype(F32).astype(BF16)
    return low, (1.0 - low.astype(F32)).astype(BF16)


def stack_heads(x, masks):
    return jnp.concatenate([x * masks[0], x * masks[1]], axis=0)


def compute(tok, cot, lens, segr, wqkv, wout, wup, wdown, small, out, ingrad, gqkv, gout, gup, gdown, gsmall,
            normed, qkv, attn, mgrad, dq, dk, dv, lse, segc, act, ul):
    rows_count = tok.shape[0]
    tiles = rows_count // TQ

    def srow(i):
        return small[i : i + 1, :]

    total = jnp.sum(lens[...], axis=-1, keepdims=True)

    R1 = 256

    def p1(i, c):
        rows = pl.ds(pl.multiple_of(i * R1, R1), R1)
        xhat, _ = normalize(tok[rows, :].astype(F32))
        n = (xhat * srow(GAIN1) + srow(BIAS1)).astype(BF16)
        normed[rows, :] = n
        qkv[rows, 0:D] = (nn(n, wqkv[:, 0:D]) + srow(BQ)).astype(BF16) * jnp.asarray(HEAD_DIM ** -0.5, BF16)
        qkv[rows, D : 2 * D] = nn(n, wqkv[:, D : 2 * D]).astype(BF16)
        qkv[rows, 2 * D : 3 * D] = (nn(n, wqkv[:, 2 * D : 3 * D]) + srow(BV)).astype(BF16)
        return c

    lax.fori_loop(0, rows_count // R1, p1, 0)

    def pseg(i, c):
        rows = pl.ds(pl.multiple_of(i * 128, 128), 128)
        segc[rows, :] = jnp.broadcast_to(segr[pl.ds(i, 1), :], (128, 128)).T
        return c

    lax.fori_loop(0, rows_count // 128, pseg, 0)

    masks = half_masks(TQ)

    def window(i):
        b = pl.multiple_of(i * TQ, TQ)
        ws = jnp.clip(b - MARGIN, 0, rows_count - WIN)
        return pl.ds(b, TQ), pl.ds(pl.multiple_of(ws, 16), WIN)

    def allowed(i, wrows):
        segk = segc[wrows, :]
        segq = jnp.broadcast_to(segr[pl.ds(i, 1), :], (WIN, 128))
        return jnp.concatenate([segk, segk], axis=1) == jnp.concatenate([segq, segq], axis=1)

    def unstack_t(x):
        return jnp.concatenate([x[:HEAD_DIM, :TQ], x[HEAD_DIM:, TQ:]], axis=0).T

    def p2(i, c):
        qrows, wrows = window(i)
        mask = allowed(i, wrows)
        for j in range(PAIRS):
            q2 = stack_heads(qkv[qrows, j * 128 : (j + 1) * 128], masks)
            kw = qkv[wrows, D + j * 128 : D + (j + 1) * 128]
            vw = qkv[wrows, 2 * D + j * 128 : 2 * D + (j + 1) * 128]
            s = jnp.where(mask, nt(kw, q2), MASKED)
            m = jnp.max(s, axis=0, keepdims=True)
            e = jnp.exp(s - m)
            l = jnp.sum(e, axis=0, keepdims=True)
            o = tn(vw, e.astype(BF16)) * (1.0 / l)
            attn[qrows, j * 128 : (j + 1) * 128] = unstack_t(o).astype(BF16)
            lse[pl.ds(i * PAIRS + j, 1), :] = m + jnp.log(l)
        return c

    lax.fori_loop(0, tiles, p2, 0)

    gout[...] = jnp.zeros_like(gout)
    gup[...] = jnp.zeros_like(gup)
    gdown[...] = jnp.zeros_like(gdown)
    gqkv[...] = jnp.zeros_like(gqkv)
    gsmall[...] = jnp.zeros_like(gsmall)
    dk[...] = jnp.zeros_like(dk)
    dv[...] = jnp.zeros_like(dv)
    R3 = act.shape[0]
    CH = 384

    def p3(i, c):
        r0 = pl.multiple_of(i * R3, R3)
        rows = pl.ds(r0, R3)
        filled = (lax.broadcasted_iota(jnp.int32, (R3, 1), 0) + r0 < total).astype(F32)
        att = attn[rows, :]
        mixed = tok[rows, :].astype(F32) + nn(att, wout[...]) + srow(BOUT)
        xhat, r = normalize(mixed)
        n2 = (xhat * srow(GAIN2) + srow(BIAS2)).astype(BF16)
        upstream = cot[rows, :].astype(F32) * filled
        up_low = upstream.astype(BF16)
        for cidx in range(FF // CH):
            cols = slice(cidx * CH, (cidx + 1) * CH)
            u = nn(n2, wup[:, cols]) + srow(BUP + cidx)
            cdf, pdf = gelu_parts(u)
            act[:, cols] = (u * cdf).astype(BF16)
            ug = nt(up_low, wdown[cols, :]) * (cdf + u * pdf)
            gsmall[BUP + cidx : BUP + cidx + 1, :] += colsum(ug)
            ul[:, cols] = ug.astype(BF16)
        res = mixed + nn(act[...], wdown[...]) + srow(BDOWN)
        out[rows, :] = (res * filled).astype(BF16)
        ng = nt(ul[...], wup[...])
        mg = upstream + norm_back(ng, srow(GAIN2), xhat, r)
        gsmall[GAIN2 : GAIN2 + 1, :] += colsum(ng * xhat)
        gsmall[BIAS2 : BIAS2 + 1, :] += colsum(ng)
        gsmall[BOUT : BOUT + 1, :] += colsum(mg)
        gsmall[BDOWN : BDOWN + 1, :] += colsum(upstream)
        mgrad[rows, :] = mg
        ml = mg.astype(BF16)
        gout[...] += tn(att, ml)
        attn[rows, :] = nt(ml, wout[...]).astype(BF16)
        for cidx in range(FF // CH):
            cols = slice(cidx * CH, (cidx + 1) * CH)
            gdown[cols, :] += tn(act[:, cols], up_low)
            gup[:, cols] += tn(n2, ul[:, cols])
        return c

    lax.fori_loop(0, rows_count // R3, p3, 0)

    def p4(i, c):
        qrows, wrows = window(i)
        mask = allowed(i, wrows)
        for j in range(PAIRS):
            cols = slice(j * 128, (j + 1) * 128)
            q2 = stack_heads(qkv[qrows, cols], masks)
            do2 = stack_heads(attn[qrows, cols], masks)
            kw = qkv[wrows, D + j * 128 : D + (j + 1) * 128]
            vw = qkv[wrows, 2 * D + j * 128 : 2 * D + (j + 1) * 128]
            s = jnp.where(mask, nt(kw, q2), MASKED)
            p = jnp.exp(s - lse[pl.ds(i * PAIRS + j, 1), :])
            dp = nt(vw, do2)
            delta = jnp.sum(p * dp, axis=0, keepdims=True)
            ds = (p * (dp - delta)).astype(BF16)
            dv[wrows, cols] += nn(p.astype(BF16), do2)
            dk[wrows, cols] += nn(ds, q2)
            dqj = unstack_t(tn(kw, ds)) * (HEAD_DIM ** -0.5)
            gsmall[BQ : BQ + 1, cols] += colsum(dqj)
            dq[qrows, cols] = dqj.astype(BF16)
        return c

    lax.fori_loop(0, tiles, p4, 0)

    R5 = 256

    def p5(i, c):
        rows = pl.ds(pl.multiple_of(i * R5, R5), R5)
        dvr = dv[rows, :]
        gsmall[BV : BV + 1, :] += colsum(dvr)
        dproj = jnp.concatenate([dq[rows, :], dk[rows, :].astype(BF16), dvr.astype(BF16)], axis=1)
        ng = nt(dproj, wqkv[...])
        xhat, r = normalize(tok[rows, :].astype(F32))
        gsmall[GAIN1 : GAIN1 + 1, :] += colsum(ng * xhat)
        gsmall[BIAS1 : BIAS1 + 1, :] += colsum(ng)
        ingrad[rows, :] = (mgrad[rows, :] + norm_back(ng, srow(GAIN1), xhat, r)).astype(BF16)
        n = normed[rows, :]
        for cidx in range(3):
            cols = slice(cidx * D, (cidx + 1) * D)
            gqkv[:, cols] += tn(n, dproj[:, cols])
        return c

    lax.fori_loop(0, rows_count // R5, p5, 0)


def run_compute(tok, cot, lens, segr, wqkv, wout, wup, wdown, small):
    rows = tok.shape[0]
    sds = jax.ShapeDtypeStruct
    vm = pl.BlockSpec(memory_space=pltpu.VMEM)
    return pl.pallas_call(
        compute,
        out_shape=(
            sds((rows, D), BF16), sds((rows, D), BF16), sds((D, 3 * D), F32), sds((D, D), F32),
            sds((D, FF), F32), sds((FF, D), F32), sds((SMALL_ROWS, D), F32),
        ),
        in_specs=[vm] * 9,
        out_specs=(vm,) * 7,
        scratch_shapes=[
            pltpu.VMEM((rows, D), BF16),
            pltpu.VMEM((rows, 3 * D), BF16),
            pltpu.VMEM((rows, D), BF16),
            pltpu.VMEM((rows, D), F32),
            pltpu.VMEM((rows, D), BF16),
            pltpu.VMEM((rows, D), F32),
            pltpu.VMEM((rows, D), F32),
            pltpu.VMEM((rows // TQ * PAIRS, 2 * TQ), F32),
            pltpu.VMEM((rows, 128), jnp.int32),
            pltpu.VMEM((256, FF), BF16),
            pltpu.VMEM((256, FF), BF16),
        ],
        compiler_params=pltpu.CompilerParams(vmem_limit_bytes=62 << 20),
        name="layer",
    )(tok, cot, lens, segr, wqkv, wout, wup, wdown, small)


def local(tokens, cotangent, image_lengths, segment_ids, w_qkv, w_out, w_up, w_down, small_params):
    axes = ("dp", "fsdp")
    gather = lambda w: lax.all_gather(w, axes, axis=0, tiled=True)
    scatter = lambda g: lax.psum_scatter(g, axes, scatter_dimension=0, tiled=True)
    wqkv = gather(w_qkv).reshape(D, 3 * D)
    wout = gather(w_out).reshape(D, D)
    wup = gather(w_up).reshape(D, FF)
    wdown = gather(w_down).reshape(FF, D)
    small = jnp.pad(gather(small_params).astype(F32).reshape(-1, D), ((0, SMALL_ROWS - 12), (0, 0)))
    out, ingrad, gqkv, gout, gup, gdown, gsmall = run_compute(
        tokens, cotangent, image_lengths, segment_ids.reshape(-1, 128), wqkv, wout, wup, wdown, small
    )
    return (
        out, ingrad, scatter(gqkv.reshape(-1)), scatter(gout.reshape(-1)), scatter(gup.reshape(-1)),
        scatter(gdown.reshape(-1)), scatter(gsmall[:12].reshape(-1)),
    )


def solution(mesh):
    both = P(("dp", "fsdp"))
    rows = P(("dp", "fsdp"), None)
    return jax.shard_map(
        local, mesh=mesh,
        in_specs=(rows, rows, rows) + (both,) * 6,
        out_specs=(rows, rows) + (both,) * 5,
        check_vma=False,
    )
```

```python
import functools

import jax
import jax.numpy as jnp
from jax import lax
from jax.experimental import pallas as pl
from jax.experimental.pallas import tpu as pltpu
from jax.sharding import PartitionSpec as P

HEADS = 6
HEAD_DIM = 64
FF = 1536
D = HEADS * HEAD_DIM
PAIRS = D // 128
MAX_IMG = 66
NORM_EPS = 1e-06
MASKED = -1e30
F32 = jnp.float32
BF16 = jnp.bfloat16

GAIN1, GAIN2, BIAS1, BIAS2, BQ, BV, BOUT, BDOWN, BUP = range(9)
SMALL_ROWS = 16

TQ = 128
MARGIN = 16 * ((MAX_IMG - 1 + 15) // 16)
WIN = TQ + 2 * MARGIN


def nn(a, b):
    return jnp.dot(a, b, preferred_element_type=F32)


def nt(a, b):
    return lax.dot_general(a, b, (((1,), (1,)), ((), ())), preferred_element_type=F32)


def tn(a, b):
    return lax.dot_general(a, b, (((0,), (0,)), ((), ())), preferred_element_type=F32)


def normalize(x):
    center = jnp.mean(x, axis=-1, keepdims=True)
    off = x - center
    r = lax.rsqrt(jnp.mean(off * off, axis=-1, keepdims=True) + NORM_EPS)
    return off * r, r


def norm_back(grad, gain, xhat, r):
    gx = grad * gain
    return r * (gx - jnp.mean(gx, axis=-1, keepdims=True) - xhat * jnp.mean(gx * xhat, axis=-1, keepdims=True))


def colsum(x):
    return jnp.sum(x, axis=0, keepdims=True)


def gelu_parts(u):
    e = jnp.exp(u * u * -0.5)
    t = 1.0 / (1.0 + jnp.abs(u) * (0.3275911 * 0.7071067811865476))
    poly = t * (0.127414796 + t * (-0.142248368 + t * (0.7107068705 + t * (-0.7265760135 + t * 0.5307027145))))
    tail = poly * e
    cdf = jnp.where(u >= 0.0, 1.0 - tail, tail)
    return cdf, e * 0.3989422804014327


def half_masks(rows):
    lane = lax.broadcasted_iota(jnp.int32, (rows, 128), 1)
    low = (lane < HEAD_DIM).astype(F32).astype(BF16)
    return low, (1.0 - low.astype(F32)).astype(BF16)


def stack_heads(x, masks):
    return jnp.concatenate([x * masks[0], x * masks[1]], axis=0)


def compute(tok, cot, lens, segr, wqkv, wout, wup, wdown, small, out, ingrad, gqkv, gout, gup, gdown, gsmall,
            normed, qkv, attn, mgrad, dq, dk, dv, lse, segc, act, ul):
    rows_count = tok.shape[0]
    tiles = rows_count // TQ

    def srow(i):
        return small[i : i + 1, :]

    total = jnp.sum(lens[...], axis=-1, keepdims=True)

    R1 = 256

    def p1(i, c):
        rows = pl.ds(pl.multiple_of(i * R1, R1), R1)
        xhat, _ = normalize(tok[rows, :].astype(F32))
        n = (xhat * srow(GAIN1) + srow(BIAS1)).astype(BF16)
        normed[rows, :] = n
        qkv[rows, 0:D] = (nn(n, wqkv[:, 0:D]) + srow(BQ)).astype(BF16) * jnp.asarray(HEAD_DIM ** -0.5, BF16)
        qkv[rows, D : 2 * D] = nn(n, wqkv[:, D : 2 * D]).astype(BF16)
        qkv[rows, 2 * D : 3 * D] = (nn(n, wqkv[:, 2 * D : 3 * D]) + srow(BV)).astype(BF16)
        return c

    lax.fori_loop(0, rows_count // R1, p1, 0)

    def pseg(i, c):
        rows = pl.ds(pl.multiple_of(i * 128, 128), 128)
        segc[rows, :] = jnp.broadcast_to(segr[pl.ds(i, 1), :], (128, 128)).T
        return c

    lax.fori_loop(0, rows_count // 128, pseg, 0)

    masks = half_masks(TQ)

    def window(i):
        b = pl.multiple_of(i * TQ, TQ)
        ws = jnp.clip(b - MARGIN, 0, rows_count - WIN)
        return pl.ds(b, TQ), pl.ds(pl.multiple_of(ws, 16), WIN)

    def allowed(i, wrows):
        segk = segc[wrows, :]
        segq = jnp.broadcast_to(segr[pl.ds(i, 1), :], (WIN, 128))
        return jnp.concatenate([segk, segk], axis=1) == jnp.concatenate([segq, segq], axis=1)

    def unstack_t(x):
        return jnp.concatenate([x[:HEAD_DIM, :TQ], x[HEAD_DIM:, TQ:]], axis=0).T

    def p2(i, c):
        qrows, wrows = window(i)
        mask = allowed(i, wrows)
        for j in range(PAIRS):
            q2 = stack_heads(qkv[qrows, j * 128 : (j + 1) * 128], masks)
            kw = qkv[wrows, D + j * 128 : D + (j + 1) * 128]
            vw = qkv[wrows, 2 * D + j * 128 : 2 * D + (j + 1) * 128]
            s = jnp.where(mask, nt(kw, q2), MASKED)
            m = jnp.max(s, axis=0, keepdims=True)
            e = jnp.exp(s - m)
            l = jnp.sum(e, axis=0, keepdims=True)
            o = tn(vw, e.astype(BF16)) * (1.0 / l)
            attn[qrows, j * 128 : (j + 1) * 128] = unstack_t(o).astype(BF16)
            lse[pl.ds(i * PAIRS + j, 1), :] = m + jnp.log(l)
        return c

    lax.fori_loop(0, tiles, p2, 0)

    gout[...] = jnp.zeros_like(gout)
    gup[...] = jnp.zeros_like(gup)
    gdown[...] = jnp.zeros_like(gdown)
    gqkv[...] = jnp.zeros_like(gqkv)
    gsmall[...] = jnp.zeros_like(gsmall)
    dk[...] = jnp.zeros_like(dk)
    dv[...] = jnp.zeros_like(dv)
    R3 = act.shape[0]
    CH = 384

    def p3(i, c):
        r0 = pl.multiple_of(i * R3, R3)
        rows = pl.ds(r0, R3)
        filled = (lax.broadcasted_iota(jnp.int32, (R3, 1), 0) + r0 < total).astype(F32)
        att = attn[rows, :]
        mixed = tok[rows, :].astype(F32) + nn(att, wout[...]) + srow(BOUT)
        xhat, r = normalize(mixed)
        n2 = (xhat * srow(GAIN2) + srow(BIAS2)).astype(BF16)
        upstream = cot[rows, :].astype(F32) * filled
        up_low = upstream.astype(BF16)
        for cidx in range(FF // CH):
            cols = slice(cidx * CH, (cidx + 1) * CH)
            u = nn(n2, wup[:, cols]) + srow(BUP + cidx)
            cdf, pdf = gelu_parts(u)
            act[:, cols] = (u * cdf).astype(BF16)
            ug = nt(up_low, wdown[cols, :]) * (cdf + u * pdf)
            gsmall[BUP + cidx : BUP + cidx + 1, :] += colsum(ug)
            ul[:, cols] = ug.astype(BF16)
        res = mixed + nn(act[...], wdown[...]) + srow(BDOWN)
        out[rows, :] = (res * filled).astype(BF16)
        ng = nt(ul[...], wup[...])
        mg = upstream + norm_back(ng, srow(GAIN2), xhat, r)
        gsmall[GAIN2 : GAIN2 + 1, :] += colsum(ng * xhat)
        gsmall[BIAS2 : BIAS2 + 1, :] += colsum(ng)
        gsmall[BOUT : BOUT + 1, :] += colsum(mg)
        gsmall[BDOWN : BDOWN + 1, :] += colsum(upstream)
        mgrad[rows, :] = mg
        ml = mg.astype(BF16)
        gout[...] += tn(att, ml)
        attn[rows, :] = nt(ml, wout[...]).astype(BF16)
        for cidx in range(FF // CH):
            cols = slice(cidx * CH, (cidx + 1) * CH)
            gdown[cols, :] += tn(act[:, cols], up_low)
            gup[:, cols] += tn(n2, ul[:, cols])
        return c

    lax.fori_loop(0, rows_count // R3, p3, 0)

    def p4(i, c):
        qrows, wrows = window(i)
        mask = allowed(i, wrows)
        for j in range(PAIRS):
            cols = slice(j * 128, (j + 1) * 128)
            q2 = stack_heads(qkv[qrows, cols], masks)
            do2 = stack_heads(attn[qrows, cols], masks)
            kw = qkv[wrows, D + j * 128 : D + (j + 1) * 128]
            vw = qkv[wrows, 2 * D + j * 128 : 2 * D + (j + 1) * 128]
            s = jnp.where(mask, nt(kw, q2), MASKED)
            p = jnp.exp(s - lse[pl.ds(i * PAIRS + j, 1), :])
            dp = nt(vw, do2)
            delta = jnp.sum(p * dp, axis=0, keepdims=True)
            ds = (p * (dp - delta)).astype(BF16)
            dv[wrows, cols] += nn(p.astype(BF16), do2)
            dk[wrows, cols] += nn(ds, q2)
            dqj = unstack_t(tn(kw, ds)) * (HEAD_DIM ** -0.5)
            gsmall[BQ : BQ + 1, cols] += colsum(dqj)
            dq[qrows, cols] = dqj.astype(BF16)
        return c

    lax.fori_loop(0, tiles, p4, 0)

    R5 = 256

    def p5(i, c):
        rows = pl.ds(pl.multiple_of(i * R5, R5), R5)
        dvr = dv[rows, :]
        gsmall[BV : BV + 1, :] += colsum(dvr)
        dproj = jnp.concatenate([dq[rows, :], dk[rows, :].astype(BF16), dvr.astype(BF16)], axis=1)
        ng = nt(dproj, wqkv[...])
        xhat, r = normalize(tok[rows, :].astype(F32))
        gsmall[GAIN1 : GAIN1 + 1, :] += colsum(ng * xhat)
        gsmall[BIAS1 : BIAS1 + 1, :] += colsum(ng)
        ingrad[rows, :] = (mgrad[rows, :] + norm_back(ng, srow(GAIN1), xhat, r)).astype(BF16)
        n = normed[rows, :]
        for cidx in range(3):
            cols = slice(cidx * D, (cidx + 1) * D)
            gqkv[:, cols] += tn(n, dproj[:, cols])
        return c

    lax.fori_loop(0, rows_count // R5, p5, 0)


def run_compute(tok, cot, lens, segr, wqkv, wout, wup, wdown, small):
    rows = tok.shape[0]
    sds = jax.ShapeDtypeStruct
    vm = pl.BlockSpec(memory_space=pltpu.VMEM)
    return pl.pallas_call(
        compute,
        out_shape=(
            sds((rows, D), BF16), sds((rows, D), BF16), sds((D, 3 * D), F32), sds((D, D), F32),
            sds((D, FF), F32), sds((FF, D), F32), sds((SMALL_ROWS, D), F32),
        ),
        in_specs=[vm] * 9,
        out_specs=(vm,) * 7,
        scratch_shapes=[
            pltpu.VMEM((rows, D), BF16),
            pltpu.VMEM((rows, 3 * D), BF16),
            pltpu.VMEM((rows, D), BF16),
            pltpu.VMEM((rows, D), F32),
            pltpu.VMEM((rows, D), BF16),
            pltpu.VMEM((rows, D), F32),
            pltpu.VMEM((rows, D), F32),
            pltpu.VMEM((rows // TQ * PAIRS, 2 * TQ), F32),
            pltpu.VMEM((rows, 128), jnp.int32),
            pltpu.VMEM((256, FF), BF16),
            pltpu.VMEM((256, FF), BF16),
        ],
        compiler_params=pltpu.CompilerParams(vmem_limit_bytes=62 << 20),
        name="layer",
    )(tok, cot, lens, segr, wqkv, wout, wup, wdown, small)


BLOCK = 160
ROWS_A = slice(0, 64)
ROWS_B = slice(64, 160)
NSEM = 11


class Place:
    def __init__(self):
        dp, f = lax.axis_index("dp"), lax.axis_index("fsdp")
        self.z, self.y = lax.div(dp, 2), lax.rem(dp, 2)
        self.x, self.c = lax.div(f, 2), lax.rem(f, 2)
        self.dp, self.f = dp, f
        self.ypeer = (self.z * 2 + 1 - self.y, f)
        self.xpeer = (dp, (1 - self.x) * 2 + self.c)
        self.cpeer = (dp, self.x * 2 + 1 - self.c)

    def zpeer(self, k):
        return (lax.rem(self.z + k, 4) * 2 + self.y, self.f)

    def peers(self):
        return [self.ypeer, self.xpeer, self.cpeer] + [self.zpeer(k) for k in (1, 2, 3)]


def greet(at):
    barrier = pltpu.get_barrier_semaphore()
    for peer in at.peers():
        pl.semaphore_signal(barrier, inc=1, device_id=peer, device_id_type=pl.DeviceIdType.MESH)
    pl.semaphore_wait(barrier, 6)


def send(src, dst, ssem, rsem, i, peer):
    return pltpu.make_async_remote_copy(
        src_ref=src, dst_ref=dst, send_sem=ssem.at[i], recv_sem=rsem.at[i],
        device_id=peer, device_id_type=pl.DeviceIdType.MESH,
    )


class Gather:
    def __init__(self, buf, rows, ssem, rsem, at):
        z, y, x, c = at.z, at.y, at.x, at.c
        whole = slice(None)

        def copy(i, peer, zs, ys, xs):
            ref = buf.at[zs, ys, xs, c, rows]
            return send(ref, ref, ssem, rsem, i, peer)

        self.zs = [copy(k - 1, at.zpeer(k), z, y, x) for k in (1, 2, 3)]
        self.own = [copy(3, at.ypeer, whole, y, x), copy(4, at.xpeer, whole, y, x), copy(5, at.cpeer, whole, y, x)]
        self.relay = [
            copy(6, at.ypeer, pl.ds(0, 2), y, 1 - x), copy(7, at.xpeer, pl.ds(2, 2), 1 - y, x),
            copy(8, at.cpeer, whole, y, 1 - x), copy(9, at.cpeer, whole, 1 - y, x),
        ]
        self.last = copy(10, at.cpeer, whole, 1 - y, 1 - x)

    def step0(self):
        for s in self.zs:
            s.start()

    def step1(self):
        for s in self.zs:
            s.wait_recv()
        for s in self.own:
            s.start()

    def step2(self):
        self.own[0].wait_recv()
        self.own[1].wait_recv()
        for s in self.relay:
            s.start()

    def step3(self):
        self.relay[0].wait_recv()
        self.relay[1].wait_recv()
        self.last.start()

    def step4(self):
        for s in (self.own[2], self.relay[2], self.relay[3], self.last):
            s.wait_recv()
        for s in self.zs + self.own + self.relay + [self.last]:
            s.wait_send()


def divide(i, by):
    return lax.shift_right_logical(i * ((65536 + by - 1) // by), 16)


def swap_matrix():
    j = lax.broadcasted_iota(jnp.int32, (192, 192), 0)
    i = lax.broadcasted_iota(jnp.int32, (192, 192), 1)
    outer = divide(i, 48)
    rest = i - 48 * outer
    inner = divide(rest, 12)
    return (j == 48 * inner + 12 * outer + (rest - 12 * inner)).astype(F32).astype(BF16)


def onehot(cond):
    return cond.astype(F32).astype(BF16)


def small_maps():
    iota = lambda shape, d: lax.broadcasted_iota(jnp.int32, shape, d)
    q, lane = iota((96, D), 0), iota((96, D), 1)
    chunk = divide(lane, 48)
    third = q - 3 * divide(q, 3)
    eighth = q - 8 * divide(q, 8)
    m1 = onehot(chunk == third)
    m2 = onehot(chunk == eighth)
    e = onehot(divide(iota((96, 32), 0), 3) == iota((96, 32), 1))
    et = onehot(divide(iota((32, 96), 1), 3) == iota((32, 96), 0))
    a = onehot(divide(iota((SMALL_ROWS, 96), 1), 8) == iota((SMALL_ROWS, 96), 0))
    at = onehot(divide(iota((96, SMALL_ROWS), 0), 8) == iota((96, SMALL_ROWS), 1))
    k, l = iota((D, D), 0), iota((D, D), 1)
    lr = onehot((k - 48 * divide(k, 48)) == (l - 48 * divide(l, 48)))
    return m1, m2, e, et, a, at, lr


def small_table(rows32):
    m1, m2, e, _, a, _, lr = small_maps()
    t = nn(e, rows32).astype(BF16) * m1
    t = nn(t, lr).astype(BF16) * m2
    return nn(a, t)


def small_rows(table):
    m1, m2, _, et, _, at, lr = small_maps()
    t = nn(at, table).astype(BF16) * m2
    t = nn(t, lr).astype(BF16) * m1
    return nn(et, t).astype(BF16)


def pack_share(block, fqkv, fout, fup, fdown, fsmall, flat, stage):
    block[0:16, :] = fsmall[...]
    for at, parts in ((16, ((fqkv, 9, 0), (fout, 3, 3))), (64, ((fup, 12, 0),))):
        for ref, per, group in parts:
            n = ref.shape[0]
            flat[0:n, :] = ref[...].astype(F32)
            for j in range(per):
                g = group + j // 3
                stage[12 * g : 12 * g + 12, (j % 3) * 128 : (j % 3 + 1) * 128] = flat[pl.ds(j, 12, stride=per), :]
        block[at : at + 48, :] = stage[...].astype(BF16)
    flat[...] = fdown[...].astype(F32)
    for j in range(3):
        block[112:160, j * 128 : (j + 1) * 128] = flat[pl.ds(j, 48, stride=3), :].astype(BF16)


def unpack_quad(buf, p, first, swap):
    z, y = lax.div(p, 2), lax.rem(p, 2)
    quad = buf[z, y, :, :, first : first + 48, :].reshape(192, D)
    return nn(swap, quad).astype(BF16)


def unpack_a(buf, swap, wqkv, wout):
    def body(p, carry):
        rows = pl.ds(pl.multiple_of(p * 48, 16), 48)
        m = unpack_quad(buf, p, 16, swap)
        for g in range(3):
            wqkv[rows, g * D : (g + 1) * D] = m[48 * g : 48 * g + 48]
        wout[rows, :] = m[144:192]
        return carry

    lax.fori_loop(0, 8, body, 0)


def unpack_b(buf, swap, wup, wdown):
    def body(p, carry):
        z, y = lax.div(p, 2), lax.rem(p, 2)
        rows = pl.ds(pl.multiple_of(p * 48, 16), 48)
        m = unpack_quad(buf, p, 64, swap)
        for g in range(4):
            wup[rows, g * D : (g + 1) * D] = m[48 * g : 48 * g + 48]
        wdown[pl.ds(pl.multiple_of(p * 192, 16), 192), :] = buf[z, y, :, :, 112:160, :].reshape(192, D)
        return carry

    lax.fori_loop(0, 8, body, 0)


def gather_kernel(fqkv, fout, fup, fdown, fsmall, wqkv, wout, wup, wdown, small, buf, flat, stage, ssem, rsem):
    at = Place()
    pack_share(buf.at[at.z, at.y, at.x, at.c], fqkv, fout, fup, fdown, fsmall, flat, stage)
    greet(at)
    ga = Gather(buf, pl.ds(0, 64), ssem.at[0], rsem.at[0], at)
    gb = Gather(buf, pl.ds(64, 96), ssem.at[1], rsem.at[1], at)
    swap = swap_matrix()
    ga.step0()
    ga.step1()
    gb.step0()
    ga.step2()
    gb.step1()
    ga.step3()
    gb.step2()
    ga.step4()
    unpack_a(buf, swap, wqkv, wout)
    small[...] = small_table(buf[:, :, :, :, 0, :].reshape(32, D))
    gb.step3()
    gb.step4()
    unpack_b(buf, swap, wup, wdown)


def run_gather(fqkv, fout, fup, fdown, fsmall):
    sds = jax.ShapeDtypeStruct
    vm = pl.BlockSpec(memory_space=pltpu.VMEM)
    return pl.pallas_call(
        gather_kernel,
        out_shape=(
            sds((D, 3 * D), BF16), sds((D, D), BF16), sds((D, FF), BF16), sds((FF, D), BF16), sds((SMALL_ROWS, D), F32),
        ),
        in_specs=[vm] * 5,
        out_specs=(vm,) * 5,
        scratch_shapes=[
            pltpu.VMEM((4, 2, 2, 2, BLOCK, D), BF16),
            pltpu.VMEM((144, 128), F32),
            pltpu.VMEM((48, D), F32),
            pltpu.SemaphoreType.DMA((2, NSEM)),
            pltpu.SemaphoreType.DMA((2, NSEM)),
        ],
        compiler_params=pltpu.CompilerParams(vmem_limit_bytes=32 << 20, collective_id=0, has_side_effects=True),
        name="gather_weights",
    )(fqkv, fout, fup, fdown, fsmall)


class Scatter:
    def __init__(self, buf, rc, rd, rn, rz, zbuf, n, ssem, rsem, at):
        self.__dict__.update(buf=buf, rc=rc, rd=rd, rn=rn, rz=rz, zbuf=zbuf, n=n, at=at)
        z, y, x, c = at.z, at.y, at.x, at.c
        lo, hi = pl.ds(0, 2), pl.ds(2, 2)
        cp = lambda i, peer, src, dst: send(src, dst, ssem, rsem, i, peer)
        self.core = cp(0, at.cpeer, buf.at[:, :, :, 1 - c], rc)
        self.diag = [
            cp(1, at.xpeer, buf.at[lo, 1 - y, 1 - x, c], rd.at[0]),
            cp(2, at.ypeer, buf.at[hi, 1 - y, 1 - x, c], rd.at[1]),
        ]
        self.early = [
            cp(3, at.ypeer, buf.at[hi, 1 - y, x, c], rn.at[0, hi]),
            cp(4, at.xpeer, buf.at[lo, y, 1 - x, c], rn.at[1, lo]),
        ]
        self.late = [
            cp(5, at.ypeer, buf.at[lo, 1 - y, x, c], rn.at[0, lo]),
            cp(6, at.xpeer, buf.at[hi, y, 1 - x, c], rn.at[1, hi]),
        ]
        self.zs = [cp(6 + k, at.zpeer(k), zbuf.at[lax.rem(z + k, 4)], rz.at[k - 1]) for k in (1, 2, 3)]

    def step0(self):
        self.core.start()

    def step1(self):
        at, buf, rc = self.at, self.buf, self.rc
        self.core.wait_recv()

        def add(y, x):
            for z in range(4):
                buf[z, y, x, at.c] = (buf[z, y, x, at.c].astype(F32) + rc[z, y, x].astype(F32)).astype(BF16)

        add(1 - at.y, 1 - at.x)
        for s in self.diag:
            s.start()
        add(1 - at.y, at.x)
        add(at.y, 1 - at.x)
        for s in self.early:
            s.start()
        add(at.y, at.x)

    def step2(self):
        at, buf, rd = self.at, self.buf, self.rd
        for s in self.diag:
            s.wait_recv()
        for i in range(2):
            a, b = (i, 1 - at.y, at.x, at.c), (2 + i, at.y, 1 - at.x, at.c)
            buf[a] = (buf[a].astype(F32) + rd[0, i].astype(F32)).astype(BF16)
            buf[b] = (buf[b].astype(F32) + rd[1, i].astype(F32)).astype(BF16)
        for s in self.late:
            s.start()

    def step3(self):
        at, buf, rn, zbuf = self.at, self.buf, self.rn, self.zbuf
        for s in self.early + self.late:
            s.wait_recv()
        for z in range(4):
            mine = buf[z, at.y, at.x, at.c].astype(F32)
            zbuf[z] = (mine + rn[0, z].astype(F32) + rn[1, z].astype(F32)).astype(BF16)
        for s in self.zs:
            s.start()

    def step4(self):
        rz, zbuf = self.rz, self.zbuf
        for s in self.zs:
            s.wait_recv()
        total = zbuf[self.at.z].astype(F32)
        for k in range(3):
            total = total + rz[k].astype(F32)
        for s in [self.core] + self.diag + self.early + self.late + self.zs:
            s.wait_send()
        return total


def pack_grads_b(buf, gup, gdown, swap, first):
    def body(p, carry):
        z, y = lax.div(p, 2), lax.rem(p, 2)
        rows = pl.ds(pl.multiple_of(p * 48, 16), 48)
        quad = jnp.concatenate([gup[rows, g * D : (g + 1) * D].astype(BF16) for g in range(4)], axis=0)
        buf[z, y, :, :, first : first + 48, :] = nn(swap, quad).astype(BF16).reshape(2, 2, 48, D)
        down = gdown[pl.ds(pl.multiple_of(p * 192, 16), 192), :].astype(BF16)
        buf[z, y, :, :, first + 48 : first + 96, :] = down.reshape(2, 2, 48, D)
        return carry

    lax.fori_loop(0, 8, body, 0)


def pack_grads_a(buf, gqkv, gout, gsmall, swap):
    rows32 = small_rows(gsmall[...].astype(BF16))
    i = lax.broadcasted_iota(jnp.int32, (512, 32), 0)
    d = lax.broadcasted_iota(jnp.int32, (512, 32), 1)
    spread = nn(onehot(i == 16 * d), rows32).astype(BF16)
    buf[:, :, :, :, 0:16, :] = spread.reshape(4, 2, 2, 2, 16, D)

    def body(p, carry):
        z, y = lax.div(p, 2), lax.rem(p, 2)
        rows = pl.ds(pl.multiple_of(p * 48, 16), 48)
        parts = [gqkv[rows, g * D : (g + 1) * D].astype(BF16) for g in range(3)] + [gout[rows, :].astype(BF16)]
        buf[z, y, :, :, 16:64, :] = nn(swap, jnp.concatenate(parts, axis=0)).astype(BF16).reshape(2, 2, 48, D)
        return carry

    lax.fori_loop(0, 8, body, 0)


def unpack_rows(total, first, per, group, ref):
    for j in range(per):
        g = group + j // 3
        ref[pl.ds(j, 12, stride=per), :] = total[first + 12 * g : first + 12 * g + 12, (j % 3) * 128 : (j % 3 + 1) * 128]


def unpack_down(total, first, ref):
    for j in range(3):
        ref[pl.ds(j, 48, stride=3), :] = total[first : first + 48, j * 128 : (j + 1) * 128]


def scatter_scratch(n):
    return [
        pltpu.VMEM((4, 2, 2, 2, n, D), BF16),
        pltpu.VMEM((4, 2, 2, n, D), BF16),
        pltpu.VMEM((2, 2, n, D), BF16),
        pltpu.VMEM((2, 4, n, D), BF16),
        pltpu.VMEM((3, n, D), BF16),
        pltpu.VMEM((4, n, D), BF16),
    ]


def scatter_kernel(gqkv, gout, gup, gdown, gsmall, oqkv, oout, oup, odown, osmall, *scratch):
    ba, bb, (ssem, rsem) = scratch[:6], scratch[6:12], scratch[12:]
    at = Place()
    greet(at)
    swap = swap_matrix()
    sa = Scatter(*ba, 64, ssem.at[0], rsem.at[0], at)
    sb = Scatter(*bb, 96, ssem.at[1], rsem.at[1], at)
    pack_grads_b(bb[0], gup, gdown, swap, 0)
    sb.step0()
    pack_grads_a(ba[0], gqkv, gout, gsmall, swap)
    sa.step0()
    sb.step1()
    sa.step1()
    sb.step2()
    sa.step2()
    sb.step3()
    sa.step3()
    tb = sb.step4()
    unpack_rows(tb, 0, 12, 0, oup)
    unpack_down(tb, 48, odown)
    ta = sa.step4()
    unpack_rows(ta, 16, 9, 0, oqkv)
    unpack_rows(ta, 16, 3, 3, oout)
    osmall[...] = ta[0:8, :]


def run_scatter(gqkv, gout, gup, gdown, gsmall):
    sds = jax.ShapeDtypeStruct
    vm = pl.BlockSpec(memory_space=pltpu.VMEM)
    return pl.pallas_call(
        scatter_kernel,
        out_shape=(
            sds((108, 128), F32), sds((36, 128), F32), sds((144, 128), F32), sds((144, 128), F32), sds((8, D), F32),
        ),
        in_specs=[vm] * 5,
        out_specs=(vm,) * 5,
        scratch_shapes=scatter_scratch(64) + scatter_scratch(96) + [
            pltpu.SemaphoreType.DMA((2, NSEM)),
            pltpu.SemaphoreType.DMA((2, NSEM)),
        ],
        compiler_params=pltpu.CompilerParams(vmem_limit_bytes=48 << 20, collective_id=1, has_side_effects=True),
        name="scatter_grads",
    )(gqkv, gout, gup, gdown, gsmall)


def lanes(flat):
    return flat.reshape(-1, 128)


def local_direct(tokens, cotangent, image_lengths, segment_ids, w_qkv, w_out, w_up, w_down, small_params):
    share = small_params.shape[0]
    fsmall = jnp.pad(small_params.reshape(1, share), ((0, 15), (0, D - share)))
    weights = run_gather(lanes(w_qkv), lanes(w_out), lanes(w_up), lanes(w_down), fsmall)
    out, ingrad, *grads = run_compute(tokens, cotangent, image_lengths, segment_ids.reshape(-1, 128), *weights)
    oqkv, oout, oup, odown, osmall = run_scatter(*grads)
    return out, ingrad, oqkv.reshape(-1), oout.reshape(-1), oup.reshape(-1), odown.reshape(-1), osmall[0, :share]


def local(tokens, cotangent, image_lengths, segment_ids, w_qkv, w_out, w_up, w_down, small_params):
    axes = ("dp", "fsdp")
    gather = lambda w: lax.all_gather(w, axes, axis=0, tiled=True)
    scatter = lambda g: lax.psum_scatter(g, axes, scatter_dimension=0, tiled=True)
    wqkv = gather(w_qkv).reshape(D, 3 * D)
    wout = gather(w_out).reshape(D, D)
    wup = gather(w_up).reshape(D, FF)
    wdown = gather(w_down).reshape(FF, D)
    small = jnp.pad(gather(small_params).astype(F32).reshape(-1, D), ((0, SMALL_ROWS - 12), (0, 0)))
    out, ingrad, gqkv, gout, gup, gdown, gsmall = run_compute(
        tokens, cotangent, image_lengths, segment_ids.reshape(-1, 128), wqkv, wout, wup, wdown, small
    )
    return (
        out, ingrad, scatter(gqkv.reshape(-1)), scatter(gout.reshape(-1)), scatter(gup.reshape(-1)),
        scatter(gdown.reshape(-1)), scatter(gsmall[:12].reshape(-1)),
    )


def solution(mesh):
    both = P(("dp", "fsdp"))
    rows = P(("dp", "fsdp"), None)
    direct = dict(mesh.shape) == {"dp": 8, "fsdp": 4}
    return jax.shard_map(
        local_direct if direct else local, mesh=mesh,
        in_specs=(rows, rows, rows) + (both,) * 6,
        out_specs=(rows, rows) + (both,) * 5,
        check_vma=False,
    )
```

```python
import functools

import jax
import jax.numpy as jnp
from jax import lax
from jax.experimental import pallas as pl
from jax.experimental.pallas import tpu as pltpu
from jax.sharding import PartitionSpec as P

HEADS = 6
HEAD_DIM = 64
FF = 1536
D = HEADS * HEAD_DIM
PAIRS = D // 128
MAX_IMG = 66
NORM_EPS = 1e-06
MASKED = -1e30
F32 = jnp.float32
BF16 = jnp.bfloat16

GAIN1, GAIN2, BIAS1, BIAS2, BQ, BV, BOUT, BDOWN, BUP = range(9)
SMALL_ROWS = 16

TQ = 128
MARGIN = 16 * ((MAX_IMG - 1 + 15) // 16)
WIN = TQ + 2 * MARGIN
R1 = 256
R3 = 256
R5 = 256
CH = 384
QSCALE = HEAD_DIM ** -0.5


def nn(a, b):
    return jnp.dot(a, b, preferred_element_type=F32)


def nt(a, b):
    return lax.dot_general(a, b, (((1,), (1,)), ((), ())), preferred_element_type=F32)


def tn(a, b):
    return lax.dot_general(a, b, (((0,), (0,)), ((), ())), preferred_element_type=F32)


def normalize(x):
    center = jnp.mean(x, axis=-1, keepdims=True)
    off = x - center
    r = lax.rsqrt(jnp.mean(off * off, axis=-1, keepdims=True) + NORM_EPS)
    return off * r, r


def norm_back(grad, gain, xhat, r):
    gx = grad * gain
    return r * (gx - jnp.mean(gx, axis=-1, keepdims=True) - xhat * jnp.mean(gx * xhat, axis=-1, keepdims=True))


def colsum(x):
    return jnp.sum(x, axis=0, keepdims=True)


def gelu_parts(u):
    e = jnp.exp(u * u * -0.5)
    t = 1.0 / (1.0 + jnp.abs(u) * (0.3275911 * 0.7071067811865476))
    poly = t * (0.127414796 + t * (-0.142248368 + t * (0.7107068705 + t * (-0.7265760135 + t * 0.5307027145))))
    tail = poly * e
    cdf = jnp.where(u >= 0.0, 1.0 - tail, tail)
    return cdf, e * 0.3989422804014327


def half_masks(rows):
    lane = lax.broadcasted_iota(jnp.int32, (rows, 128), 1)
    low = (lane < HEAD_DIM).astype(F32).astype(BF16)
    return low, (1.0 - low.astype(F32)).astype(BF16)


def stack_heads(x, masks):
    return jnp.concatenate([x * masks[0], x * masks[1]], axis=0)


class Layer:
    def __init__(self, **refs):
        self.__dict__.update(refs)
        self.rows_count = self.tok.shape[0]
        self.tiles = self.rows_count // TQ

    def srow(self, i):
        return self.small[i : i + 1, :]

    def loop(self, n, body, at=()):
        def step(i, carry):
            body(i)
            for k, action in at:
                pl.when(i == k)(action)
            return carry

        lax.fori_loop(0, n, step, 0)

    def norm_one(self, i):
        rows = pl.ds(pl.multiple_of(i * R1, R1), R1)
        self.mgrad[rows, :] = normalize(self.tok[rows, :].astype(F32))[0]

    def clear(self):
        for ref in (self.gout, self.gup, self.gdown, self.gqkv, self.gsmall):
            ref[...] = jnp.zeros_like(ref)

    def clear_rows(self, i):
        rows = pl.ds(pl.multiple_of(i * 16, 16), 16)
        self.dk[rows, :] = jnp.zeros((16, D), F32)
        self.dv[rows, :] = jnp.zeros((16, D), F32)

    def margins(self):
        n = self.rows_count
        for lo in (0, MARGIN + n):
            self.qkv[lo : lo + MARGIN, :] = jnp.zeros((MARGIN, 3 * D), BF16)
            self.segc[lo : lo + MARGIN, :] = jnp.full((MARGIN, 128), -1, jnp.int32)

    def segments(self, i):
        rows = pl.ds(pl.multiple_of(i * 128 + MARGIN, 16), 128)
        self.segc[rows, :] = jnp.broadcast_to(self.segr[pl.ds(i, 1), :], (128, 128)).T

    def project(self, i):
        rows = pl.ds(pl.multiple_of(i * R1, R1), R1)
        prow = pl.ds(pl.multiple_of(i * R1 + MARGIN, 16), R1)
        n = (self.mgrad[rows, :] * self.srow(GAIN1) + self.srow(BIAS1)).astype(BF16)
        self.normed[rows, :] = n
        w, out = self.wqkv, self.qkv
        out[prow, 0:D] = (nn(n, w[:, 0:D]) + self.srow(BQ)).astype(BF16) * jnp.asarray(QSCALE, BF16)
        out[prow, D : 2 * D] = nn(n, w[:, D : 2 * D]).astype(BF16)
        out[prow, 2 * D : 3 * D] = (nn(n, w[:, 2 * D : 3 * D]) + self.srow(BV)).astype(BF16)

    def window(self, i):
        b = i * TQ
        return (
            pl.ds(pl.multiple_of(b, TQ), TQ), pl.ds(pl.multiple_of(b + MARGIN, 16), TQ),
            pl.ds(pl.multiple_of(b, 16), WIN),
        )

    def allowed(self, i, wrows):
        segk = self.segc[wrows, :]
        segq = jnp.broadcast_to(self.segr[pl.ds(i, 1), :], (WIN, 128))
        return jnp.concatenate([segk, segk], axis=1) == jnp.concatenate([segq, segq], axis=1)

    @staticmethod
    def unstack_t(x):
        return jnp.concatenate([x[:HEAD_DIM, :TQ], x[HEAD_DIM:, TQ:]], axis=0).T

    def attend(self, i):
        masks = half_masks(TQ)
        orows, qrows, wrows = self.window(i)
        mask = self.allowed(i, wrows)
        for j in range(PAIRS):
            q2 = stack_heads(self.qkv[qrows, j * 128 : (j + 1) * 128], masks)
            kw = self.qkv[wrows, D + j * 128 : D + (j + 1) * 128]
            vw = self.qkv[wrows, 2 * D + j * 128 : 2 * D + (j + 1) * 128]
            s = jnp.where(mask, nt(kw, q2), MASKED)
            m = jnp.max(s, axis=0, keepdims=True)
            e = jnp.exp(s - m)
            l = jnp.sum(e, axis=0, keepdims=True)
            o = tn(vw, e.astype(BF16)) * (1.0 / l)
            self.attn[orows, j * 128 : (j + 1) * 128] = self.unstack_t(o).astype(BF16)
            self.lse[pl.ds(i * PAIRS + j, 1), :] = m + jnp.log(l)

    def feed(self, i):
        act, ul, gsmall, wout, wup, wdown = self.act, self.ul, self.gsmall, self.wout, self.wup, self.wdown
        r0 = pl.multiple_of(i * R3, R3)
        rows = pl.ds(r0, R3)
        total = jnp.sum(self.lens[...], axis=-1, keepdims=True)
        filled = (lax.broadcasted_iota(jnp.int32, (R3, 1), 0) + r0 < total).astype(F32)
        att = self.attn[rows, :]
        mixed = self.tok[rows, :].astype(F32) + nn(att, wout[...]) + self.srow(BOUT)
        xhat, r = normalize(mixed)
        n2 = (xhat * self.srow(GAIN2) + self.srow(BIAS2)).astype(BF16)
        upstream = self.cot[rows, :].astype(F32) * filled
        up_low = upstream.astype(BF16)
        for k in range(FF // CH):
            cols = slice(k * CH, (k + 1) * CH)
            u = nn(n2, wup[:, cols]) + self.srow(BUP + k)
            cdf, pdf = gelu_parts(u)
            act[:, cols] = (u * cdf).astype(BF16)
            ug = nt(up_low, wdown[cols, :]) * (cdf + u * pdf)
            gsmall[BUP + k : BUP + k + 1, :] += colsum(ug)
            ul[:, cols] = ug.astype(BF16)
        res = mixed + nn(act[...], wdown[...]) + self.srow(BDOWN)
        self.out[rows, :] = (res * filled).astype(BF16)
        ng = nt(ul[...], wup[...])
        mg = upstream + norm_back(ng, self.srow(GAIN2), xhat, r)
        gsmall[GAIN2 : GAIN2 + 1, :] += colsum(ng * xhat)
        gsmall[BIAS2 : BIAS2 + 1, :] += colsum(ng)
        gsmall[BOUT : BOUT + 1, :] += colsum(mg)
        gsmall[BDOWN : BDOWN + 1, :] += colsum(upstream)
        self.mgrad[rows, :] = mg
        ml = mg.astype(BF16)
        self.gout[...] += tn(att, ml)
        self.attn[rows, :] = nt(ml, wout[...]).astype(BF16)
        for k in range(FF // CH):
            cols = slice(k * CH, (k + 1) * CH)
            self.gdown[cols, :] += tn(act[:, cols], up_low)
            self.gup[:, cols] += tn(n2, ul[:, cols])

    def attend_back(self, i):
        masks = half_masks(TQ)
        orows, qrows, wrows = self.window(i)
        mask = self.allowed(i, wrows)
        for j in range(PAIRS):
            cols = slice(j * 128, (j + 1) * 128)
            q2 = stack_heads(self.qkv[qrows, cols], masks)
            do2 = stack_heads(self.attn[orows, cols], masks)
            kw = self.qkv[wrows, D + j * 128 : D + (j + 1) * 128]
            vw = self.qkv[wrows, 2 * D + j * 128 : 2 * D + (j + 1) * 128]
            s = jnp.where(mask, nt(kw, q2), MASKED)
            p = jnp.exp(s - self.lse[pl.ds(i * PAIRS + j, 1), :])
            dp = nt(vw, do2)
            delta = jnp.sum(p * dp, axis=0, keepdims=True)
            ds = (p * (dp - delta)).astype(BF16)
            self.dv[wrows, cols] += nn(p.astype(BF16), do2)
            self.dk[wrows, cols] += nn(ds, q2)
            dqj = self.unstack_t(tn(kw, ds)) * QSCALE
            self.gsmall[BQ : BQ + 1, cols] += colsum(dqj)
            self.dq[orows, cols] = dqj.astype(BF16)

    def project_grad(self, i):
        rows = pl.ds(pl.multiple_of(i * R5, R5), R5)
        prow = pl.ds(pl.multiple_of(i * R5 + MARGIN, 16), R5)
        dvr = self.dv[prow, :]
        self.gsmall[BV : BV + 1, :] += colsum(dvr)
        n = self.normed[rows, :]
        for k, part in enumerate((self.dq[rows, :], self.dk[prow, :].astype(BF16), dvr.astype(BF16))):
            cols = slice(k * D, (k + 1) * D)
            self.qkv[prow, cols] = part
            self.gqkv[:, cols] += tn(n, part)

    def project_back(self, i):
        rows = pl.ds(pl.multiple_of(i * R5, R5), R5)
        prow = pl.ds(pl.multiple_of(i * R5 + MARGIN, 16), R5)
        ng = nt(self.qkv[prow, :], self.wqkv[...])
        xhat, r = normalize(self.tok[rows, :].astype(F32))
        self.gsmall[GAIN1 : GAIN1 + 1, :] += colsum(ng * xhat)
        self.gsmall[BIAS1 : BIAS1 + 1, :] += colsum(ng)
        self.ingrad[rows, :] = (self.mgrad[rows, :] + norm_back(ng, self.srow(GAIN1), xhat, r)).astype(BF16)


def layer_scratch(rows):
    padded = rows + 2 * MARGIN
    return dict(
        normed=pltpu.VMEM((rows, D), BF16), qkv=pltpu.VMEM((padded, 3 * D), BF16), attn=pltpu.VMEM((rows, D), BF16),
        mgrad=pltpu.VMEM((rows, D), F32), dq=pltpu.VMEM((rows, D), BF16), dk=pltpu.VMEM((padded, D), F32),
        dv=pltpu.VMEM((padded, D), F32), lse=pltpu.VMEM((rows // TQ * PAIRS, 2 * TQ), F32),
        segc=pltpu.VMEM((padded, 128), jnp.int32), act=pltpu.VMEM((R3, FF), BF16), ul=pltpu.VMEM((R3, FF), BF16),
    )


def named_call(body, ins, outs, scratch, **options):
    names = list(ins) + list(outs) + list(scratch)

    def kernel(*refs):
        body(**dict(zip(names, refs)))

    spec = lambda space: pl.BlockSpec(memory_space=space)
    return pl.pallas_call(
        kernel,
        out_shape=tuple(jax.ShapeDtypeStruct(*shape) for shape, _ in outs.values()),
        in_specs=[spec(space) for _, space in ins.values()],
        out_specs=tuple(spec(space) for _, space in outs.values()),
        scratch_shapes=list(scratch.values()),
        **options,
    )(*(array for array, _ in ins.values()))


def alone(**refs):
    layer = Layer(**refs)
    rows = layer.rows_count
    layer.loop(rows // R1, layer.norm_one)
    layer.clear()
    layer.loop((rows + 2 * MARGIN) // 16, layer.clear_rows)
    layer.margins()
    layer.loop(rows // 128, layer.segments)
    layer.loop(rows // R1, layer.project)
    layer.loop(layer.tiles, layer.attend)
    layer.loop(rows // R3, layer.feed)
    layer.loop(layer.tiles, layer.attend_back)
    layer.loop(rows // R5, layer.project_grad)
    layer.loop(rows // R5, layer.project_back)


def run_alone(tok, cot, lens, segr, wqkv, wout, wup, wdown, small):
    rows = tok.shape[0]
    vm = pltpu.VMEM
    arrays = dict(tok=tok, cot=cot, lens=lens, segr=segr, wqkv=wqkv, wout=wout, wup=wup, wdown=wdown, small=small)
    outs = dict(
        out=((rows, D), BF16), ingrad=((rows, D), BF16), gqkv=((D, 3 * D), F32), gout=((D, D), F32),
        gup=((D, FF), F32), gdown=((FF, D), F32), gsmall=((SMALL_ROWS, D), F32),
    )
    return named_call(
        alone, {k: (v, vm) for k, v in arrays.items()}, {k: (v, vm) for k, v in outs.items()}, layer_scratch(rows),
        compiler_params=pltpu.CompilerParams(vmem_limit_bytes=62 << 20), name="layer",
    )


BLOCK = 160
ROWS_A = slice(0, 64)
ROWS_B = slice(64, 160)
NSEM = 11


class Place:
    def __init__(self):
        dp, f = lax.axis_index("dp"), lax.axis_index("fsdp")
        self.z, self.y = lax.div(dp, 2), lax.rem(dp, 2)
        self.x, self.c = lax.div(f, 2), lax.rem(f, 2)
        self.dp, self.f = dp, f
        self.ypeer = (self.z * 2 + 1 - self.y, f)
        self.xpeer = (dp, (1 - self.x) * 2 + self.c)
        self.cpeer = (dp, self.x * 2 + 1 - self.c)

    def zpeer(self, k):
        return (lax.rem(self.z + k, 4) * 2 + self.y, self.f)

    def peers(self):
        return [self.ypeer, self.xpeer, self.cpeer] + [self.zpeer(k) for k in (1, 2, 3)]


def greet(at):
    barrier = pltpu.get_barrier_semaphore()
    for peer in at.peers():
        pl.semaphore_signal(barrier, inc=1, device_id=peer, device_id_type=pl.DeviceIdType.MESH)
    pl.semaphore_wait(barrier, 6)


def send(src, dst, ssem, rsem, i, peer):
    return pltpu.make_async_remote_copy(
        src_ref=src, dst_ref=dst, send_sem=ssem.at[i], recv_sem=rsem.at[i],
        device_id=peer, device_id_type=pl.DeviceIdType.MESH,
    )


class Gather:
    def __init__(self, buf, rows, ssem, rsem, at):
        z, y, x, c = at.z, at.y, at.x, at.c
        whole = slice(None)

        def copy(i, peer, zs, ys, xs):
            ref = buf.at[zs, ys, xs, c, rows]
            return send(ref, ref, ssem, rsem, i, peer)

        self.zs = [copy(k - 1, at.zpeer(k), z, y, x) for k in (1, 2, 3)]
        self.own = [copy(3, at.ypeer, whole, y, x), copy(4, at.xpeer, whole, y, x), copy(5, at.cpeer, whole, y, x)]
        self.relay = [
            copy(6, at.ypeer, pl.ds(0, 2), y, 1 - x), copy(7, at.xpeer, pl.ds(2, 2), 1 - y, x),
            copy(8, at.cpeer, whole, y, 1 - x), copy(9, at.cpeer, whole, 1 - y, x),
        ]
        self.last = copy(10, at.cpeer, whole, 1 - y, 1 - x)

    def step0(self):
        for s in self.zs:
            s.start()

    def step1(self):
        for s in self.zs:
            s.wait_recv()
        for s in self.own:
            s.start()

    def step2(self):
        self.own[0].wait_recv()
        self.own[1].wait_recv()
        for s in self.relay:
            s.start()

    def step3(self):
        self.relay[0].wait_recv()
        self.relay[1].wait_recv()
        self.last.start()

    def step4(self):
        for s in (self.own[2], self.relay[2], self.relay[3], self.last):
            s.wait_recv()
        for s in self.zs + self.own + self.relay + [self.last]:
            s.wait_send()


def divide(i, by):
    return lax.shift_right_logical(i * ((65536 + by - 1) // by), 16)


def swap_matrix():
    j = lax.broadcasted_iota(jnp.int32, (192, 192), 0)
    i = lax.broadcasted_iota(jnp.int32, (192, 192), 1)
    outer = divide(i, 48)
    rest = i - 48 * outer
    inner = divide(rest, 12)
    return (j == 48 * inner + 12 * outer + (rest - 12 * inner)).astype(F32).astype(BF16)


def onehot(cond):
    return cond.astype(F32).astype(BF16)


def small_maps():
    iota = lambda shape, d: lax.broadcasted_iota(jnp.int32, shape, d)
    q, lane = iota((96, D), 0), iota((96, D), 1)
    chunk = divide(lane, 48)
    third = q - 3 * divide(q, 3)
    eighth = q - 8 * divide(q, 8)
    m1 = onehot(chunk == third)
    m2 = onehot(chunk == eighth)
    e = onehot(divide(iota((96, 32), 0), 3) == iota((96, 32), 1))
    et = onehot(divide(iota((32, 96), 1), 3) == iota((32, 96), 0))
    a = onehot(divide(iota((SMALL_ROWS, 96), 1), 8) == iota((SMALL_ROWS, 96), 0))
    at = onehot(divide(iota((96, SMALL_ROWS), 0), 8) == iota((96, SMALL_ROWS), 1))
    k, l = iota((D, D), 0), iota((D, D), 1)
    lr = onehot((k - 48 * divide(k, 48)) == (l - 48 * divide(l, 48)))
    return m1, m2, e, et, a, at, lr


def small_table(rows32):
    m1, m2, e, _, a, _, lr = small_maps()
    t = nn(e, rows32).astype(BF16) * m1
    t = nn(t, lr).astype(BF16) * m2
    return nn(a, t)


def small_rows(table):
    m1, m2, _, et, _, at, lr = small_maps()
    t = nn(at, table).astype(BF16) * m2
    t = nn(t, lr).astype(BF16) * m1
    return nn(et, t).astype(BF16)


def pack_share(block, what, flat, stage):
    for at, parts in what:
        for ref, per, group in parts:
            n = ref.shape[0]
            flat[0:n, :] = ref[...].astype(F32)
            for j in range(per):
                g = group + j // 3
                stage[12 * g : 12 * g + 12, (j % 3) * 128 : (j % 3 + 1) * 128] = flat[pl.ds(j, 12, stride=per), :]
        block[at : at + 48, :] = stage[...].astype(BF16)


def pack_down(block, fdown, flat):
    flat[...] = fdown[...].astype(F32)
    for j in range(3):
        block[112:160, j * 128 : (j + 1) * 128] = flat[pl.ds(j, 48, stride=3), :].astype(BF16)


def unpack_quad(buf, p, first, swap):
    z, y = lax.div(p, 2), lax.rem(p, 2)
    quad = buf[z, y, :, :, first : first + 48, :].reshape(192, D)
    return nn(swap, quad).astype(BF16)


def unpack_a(buf, swap, wqkv, wout):
    def body(p, carry):
        rows = pl.ds(pl.multiple_of(p * 48, 16), 48)
        m = unpack_quad(buf, p, 16, swap)
        for g in range(3):
            wqkv[rows, g * D : (g + 1) * D] = m[48 * g : 48 * g + 48]
        wout[rows, :] = m[144:192]
        return carry

    lax.fori_loop(0, 8, body, 0)


def unpack_b(buf, swap, wup, wdown):
    def body(p, carry):
        z, y = lax.div(p, 2), lax.rem(p, 2)
        rows = pl.ds(pl.multiple_of(p * 48, 16), 48)
        m = unpack_quad(buf, p, 64, swap)
        for g in range(4):
            wup[rows, g * D : (g + 1) * D] = m[48 * g : 48 * g + 48]
        wdown[pl.ds(pl.multiple_of(p * 192, 16), 192), :] = buf[z, y, :, :, 112:160, :].reshape(192, D)
        return carry

    lax.fori_loop(0, 8, body, 0)


class Scatter:
    def __init__(self, buf, rc, rd, rn, rz, zbuf, n, ssem, rsem, at):
        self.__dict__.update(buf=buf, rc=rc, rd=rd, rn=rn, rz=rz, zbuf=zbuf, n=n, at=at)
        z, y, x, c = at.z, at.y, at.x, at.c
        lo, hi = pl.ds(0, 2), pl.ds(2, 2)
        cp = lambda i, peer, src, dst: send(src, dst, ssem, rsem, i, peer)
        self.core = cp(0, at.cpeer, buf.at[:, :, :, 1 - c], rc)
        self.diag = [
            cp(1, at.xpeer, buf.at[lo, 1 - y, 1 - x, c], rd.at[0]),
            cp(2, at.ypeer, buf.at[hi, 1 - y, 1 - x, c], rd.at[1]),
        ]
        self.early = [
            cp(3, at.ypeer, buf.at[hi, 1 - y, x, c], rn.at[0, hi]),
            cp(4, at.xpeer, buf.at[lo, y, 1 - x, c], rn.at[1, lo]),
        ]
        self.late = [
            cp(5, at.ypeer, buf.at[lo, 1 - y, x, c], rn.at[0, lo]),
            cp(6, at.xpeer, buf.at[hi, y, 1 - x, c], rn.at[1, hi]),
        ]
        self.zs = [cp(6 + k, at.zpeer(k), zbuf.at[lax.rem(z + k, 4)], rz.at[k - 1]) for k in (1, 2, 3)]

    def step0(self):
        self.core.start()

    def step1(self):
        at, buf, rc = self.at, self.buf, self.rc
        self.core.wait_recv()

        def add(y, x):
            for z in range(4):
                buf[z, y, x, at.c] = (buf[z, y, x, at.c].astype(F32) + rc[z, y, x].astype(F32)).astype(BF16)

        add(1 - at.y, 1 - at.x)
        for s in self.diag:
            s.start()
        add(1 - at.y, at.x)
        add(at.y, 1 - at.x)
        for s in self.early:
            s.start()
        add(at.y, at.x)

    def step2(self):
        at, buf, rd = self.at, self.buf, self.rd
        for s in self.diag:
            s.wait_recv()
        for i in range(2):
            a, b = (i, 1 - at.y, at.x, at.c), (2 + i, at.y, 1 - at.x, at.c)
            buf[a] = (buf[a].astype(F32) + rd[0, i].astype(F32)).astype(BF16)
            buf[b] = (buf[b].astype(F32) + rd[1, i].astype(F32)).astype(BF16)
        for s in self.late:
            s.start()

    def step3(self):
        at, buf, rn, zbuf = self.at, self.buf, self.rn, self.zbuf
        for s in self.early + self.late:
            s.wait_recv()
        for z in range(4):
            mine = buf[z, at.y, at.x, at.c].astype(F32)
            zbuf[z] = (mine + rn[0, z].astype(F32) + rn[1, z].astype(F32)).astype(BF16)
        for s in self.zs:
            s.start()

    def step4(self):
        rz, zbuf = self.rz, self.zbuf
        for s in self.zs:
            s.wait_recv()
        total = zbuf[self.at.z].astype(F32)
        for k in range(3):
            total = total + rz[k].astype(F32)
        for s in [self.core] + self.diag + self.early + self.late + self.zs:
            s.wait_send()
        return total


def pack_grads_b(buf, gup, gdown, swap, first):
    def body(p, carry):
        z, y = lax.div(p, 2), lax.rem(p, 2)
        rows = pl.ds(pl.multiple_of(p * 48, 16), 48)
        quad = jnp.concatenate([gup[rows, g * D : (g + 1) * D].astype(BF16) for g in range(4)], axis=0)
        buf[z, y, :, :, first : first + 48, :] = nn(swap, quad).astype(BF16).reshape(2, 2, 48, D)
        down = gdown[pl.ds(pl.multiple_of(p * 192, 16), 192), :].astype(BF16)
        buf[z, y, :, :, first + 48 : first + 96, :] = down.reshape(2, 2, 48, D)
        return carry

    lax.fori_loop(0, 8, body, 0)


def pack_grads_small(buf, gsmall):
    rows32 = small_rows(gsmall[...].astype(BF16))
    i = lax.broadcasted_iota(jnp.int32, (512, 32), 0)
    d = lax.broadcasted_iota(jnp.int32, (512, 32), 1)
    buf[...] = nn(onehot(i == 16 * d), rows32).astype(BF16).reshape(4, 2, 2, 2, 16, D)


def pack_grads_a(buf, gqkv, gout, swap):
    def body(p, carry):
        z, y = lax.div(p, 2), lax.rem(p, 2)
        rows = pl.ds(pl.multiple_of(p * 48, 16), 48)
        parts = [gqkv[rows, g * D : (g + 1) * D].astype(BF16) for g in range(3)] + [gout[rows, :].astype(BF16)]
        buf[z, y] = nn(swap, jnp.concatenate(parts, axis=0)).astype(BF16).reshape(2, 2, 48, D)
        return carry

    lax.fori_loop(0, 8, body, 0)


def unpack_rows(total, first, per, group, ref):
    for j in range(per):
        g = group + j // 3
        ref[pl.ds(j, 12, stride=per), :] = total[first + 12 * g : first + 12 * g + 12, (j % 3) * 128 : (j % 3 + 1) * 128]


def unpack_down(total, first, ref):
    for j in range(3):
        ref[pl.ds(j, 48, stride=3), :] = total[first : first + 48, j * 128 : (j + 1) * 128]


def scatter_scratch(n):
    return [
        pltpu.VMEM((4, 2, 2, 2, n, D), BF16),
        pltpu.VMEM((4, 2, 2, n, D), BF16),
        pltpu.VMEM((2, 2, n, D), BF16),
        pltpu.VMEM((2, 4, n, D), BF16),
        pltpu.VMEM((3, n, D), BF16),
        pltpu.VMEM((4, n, D), BF16),
    ]


def together(tok_hbm, cot_hbm, fqkv, fout, fup, fdown, fsmall, oqkv, oout, oup, odown, osmall, **refs):
    gbuf, flat, stage, ssem, rsem, csem = (refs.pop(k) for k in ("gbuf", "flat", "stage", "ssem", "rsem", "csem"))
    scratch = lambda name: [refs.pop(name + str(i)) for i in range(6)]
    sets = {name: scratch(name) for name in "abs"}
    layer = Layer(**refs)
    rows = layer.rows_count
    at = Place()
    tok_copy = pltpu.make_async_copy(tok_hbm, layer.tok, csem.at[0])
    cot_copy = pltpu.make_async_copy(cot_hbm, layer.cot, csem.at[1])
    tok_copy.start()
    cot_copy.start()
    block = gbuf.at[at.z, at.y, at.x, at.c]
    block[0:16, :] = fsmall[...]
    pack_share(block, ((16, ((fqkv, 9, 0), (fout, 3, 3))),), flat, stage)
    greet(at)
    ga = Gather(gbuf, pl.ds(0, 64), ssem.at[0], rsem.at[0], at)
    gb = Gather(gbuf, pl.ds(64, 96), ssem.at[1], rsem.at[1], at)
    sb = Scatter(*sets["b"], 96, ssem.at[2], rsem.at[2], at)
    sa = Scatter(*sets["a"], 48, ssem.at[3], rsem.at[3], at)
    ss = Scatter(*sets["s"], 16, ssem.at[4], rsem.at[4], at)
    ga.step0()
    pack_share(block, ((64, ((fup, 12, 0),)),), flat, stage)
    pack_down(block, fdown, flat)
    swap = swap_matrix()
    tok_copy.wait()
    layer.loop(rows // R1, layer.norm_one, ((3, ga.step1), (6, gb.step0)))
    layer.margins()
    layer.loop(rows // 128, layer.segments)
    ga.step2()
    layer.clear()
    ga.step3()
    layer.loop((rows + 2 * MARGIN) // 16, layer.clear_rows)
    ga.step4()
    unpack_a(gbuf, swap, layer.wqkv, layer.wout)
    layer.small[...] = small_table(gbuf[:, :, :, :, 0, :].reshape(32, D))
    gb.step1()
    layer.loop(rows // R1, layer.project)
    layer.loop(layer.tiles, layer.attend, ((2, gb.step2), (7, gb.step3), (12, gb.step4)))
    unpack_b(gbuf, swap, layer.wup, layer.wdown)
    cot_copy.wait()
    layer.loop(rows // R3, layer.feed)
    pack_grads_b(sets["b"][0], layer.gup, layer.gdown, swap, 0)
    sb.step0()

    def finish_b():
        total = sb.step4()
        unpack_rows(total, 0, 12, 0, oup)
        unpack_down(total, 48, odown)

    layer.loop(layer.tiles, layer.attend_back, ((3, sb.step1), (6, sb.step2), (10, sb.step3), (14, finish_b)))
    layer.loop(rows // R5, layer.project_grad)
    pack_grads_a(sets["a"][0], layer.gqkv, layer.gout, swap)
    sa.step0()
    layer.loop(rows // R5, layer.project_back, ((3, sa.step1),))
    pack_grads_small(sets["s"][0], layer.gsmall)
    ss.step0()
    sa.step2()
    ss.step1()
    sa.step3()
    ss.step2()
    ss.step3()
    total = sa.step4()
    unpack_rows(total, 0, 9, 0, oqkv)
    unpack_rows(total, 0, 3, 3, oout)
    osmall[...] = ss.step4()[0:8, :]


def run_together(tok, cot, lens, segr, fqkv, fout, fup, fdown, fsmall):
    rows = tok.shape[0]
    vm, hbm = pltpu.VMEM, pl.ANY
    ins = dict(
        tok_hbm=(tok, hbm), cot_hbm=(cot, hbm), lens=(lens, vm), segr=(segr, vm), fqkv=(fqkv, vm), fout=(fout, vm),
        fup=(fup, vm), fdown=(fdown, vm), fsmall=(fsmall, vm),
    )
    outs = dict(
        out=((rows, D), BF16), ingrad=((rows, D), BF16), oqkv=(fqkv.shape, F32), oout=(fout.shape, F32),
        oup=(fup.shape, F32), odown=(fdown.shape, F32), osmall=((8, D), F32),
    )
    scratch = layer_scratch(rows) | dict(
        tok=vm((rows, D), BF16), cot=vm((rows, D), BF16), wqkv=vm((D, 3 * D), BF16), wout=vm((D, D), BF16),
        wup=vm((D, FF), BF16), wdown=vm((FF, D), BF16), small=vm((SMALL_ROWS, D), F32), gqkv=vm((D, 3 * D), F32),
        gout=vm((D, D), F32), gup=vm((D, FF), F32), gdown=vm((FF, D), F32), gsmall=vm((SMALL_ROWS, D), F32),
        gbuf=vm((4, 2, 2, 2, BLOCK, D), BF16), flat=vm((144, 128), F32), stage=vm((48, D), F32),
        ssem=pltpu.SemaphoreType.DMA((5, NSEM)), rsem=pltpu.SemaphoreType.DMA((5, NSEM)),
        csem=pltpu.SemaphoreType.DMA((2,)),
    )
    for name, n in (("a", 48), ("b", 96), ("s", 16)):
        scratch |= {name + str(i): ref for i, ref in enumerate(scatter_scratch(n))}
    return named_call(
        together, ins, {k: (v, vm) for k, v in outs.items()}, scratch,
        compiler_params=pltpu.CompilerParams(vmem_limit_bytes=63 << 20, collective_id=0, has_side_effects=True),
        name="layer_and_transfers",
    )


def lanes(flat):
    return flat.reshape(-1, 128)


def local_direct(tokens, cotangent, image_lengths, segment_ids, w_qkv, w_out, w_up, w_down, small_params):
    share = small_params.shape[0]
    fsmall = jnp.pad(small_params.reshape(1, share), ((0, 15), (0, D - share)))
    out, ingrad, oqkv, oout, oup, odown, osmall = run_together(
        tokens, cotangent, image_lengths, lanes(segment_ids), lanes(w_qkv), lanes(w_out), lanes(w_up), lanes(w_down), fsmall
    )
    return out, ingrad, oqkv.reshape(-1), oout.reshape(-1), oup.reshape(-1), odown.reshape(-1), osmall[0, :share]


def local(tokens, cotangent, image_lengths, segment_ids, w_qkv, w_out, w_up, w_down, small_params):
    axes = ("dp", "fsdp")
    gather = lambda w: lax.all_gather(w, axes, axis=0, tiled=True)
    scatter = lambda g: lax.psum_scatter(g, axes, scatter_dimension=0, tiled=True)
    wqkv = gather(w_qkv).reshape(D, 3 * D)
    wout = gather(w_out).reshape(D, D)
    wup = gather(w_up).reshape(D, FF)
    wdown = gather(w_down).reshape(FF, D)
    small = jnp.pad(gather(small_params).astype(F32).reshape(-1, D), ((0, SMALL_ROWS - 12), (0, 0)))
    out, ingrad, gqkv, gout, gup, gdown, gsmall = run_alone(
        tokens, cotangent, image_lengths, segment_ids.reshape(-1, 128), wqkv, wout, wup, wdown, small
    )
    return (
        out, ingrad, scatter(gqkv.reshape(-1)), scatter(gout.reshape(-1)), scatter(gup.reshape(-1)),
        scatter(gdown.reshape(-1)), scatter(gsmall[:12].reshape(-1)),
    )


def solution(mesh):
    both = P(("dp", "fsdp"))
    rows = P(("dp", "fsdp"), None)
    direct = dict(mesh.shape) == {"dp": 8, "fsdp": 4}
    return jax.shard_map(
        local_direct if direct else local, mesh=mesh,
        in_specs=(rows, rows, rows) + (both,) * 6,
        out_specs=(rows, rows) + (both,) * 5,
        check_vma=False,
    )
```
